32 devices in a mesh: dp: 4 (over y, x), tensor: 8 (over z, core).
Axes of the slice: x: 2, y: 2, z: 4, core: 2. Of those that a mesh axis runs over, the one named last changes fastest.
Arguments:
- inputs: bfloat16 [2, 12288, 1024], P(None, ('dp', 'tensor')), may hold values from -6 to 6
- cotangent: bfloat16 [2, 12288, 1024], P(None, ('dp', 'tensor')), may hold values from -6 to 6
- norm_gains: bfloat16 [2, 2, 1024], P(None, None, 'dp'), may hold values from 0.5 to 1.5
- norm_shifts: bfloat16 [2, 4, 1024], P(None, None, 'dp'), may hold values from -2.5 to 2.5
- project_in: bfloat16 [2, 1024, 16, 192], P(None, 'dp', 'tensor'), may hold values from -0.1875 to 0.1875
- bias_in: bfloat16 [2, 16, 128], P(None, 'tensor', 'dp'), may hold values from -1.5 to 1.5
- project_out: bfloat16 [2, 16, 64, 1024], P(None, 'tensor', None, 'dp'), may hold values from -0.75 to 0.75
- up_weight: bfloat16 [2, 1024, 4096], P(None, 'dp', 'tensor'), may hold values from -0.1875 to 0.1875
- up_bias: bfloat16 [2, 16, 256], P(None, 'tensor', 'dp'), may hold values from -2.5 to 2.5
- down_weight: bfloat16 [2, 4096, 1024], P(None, 'tensor', 'dp'), may hold values from -0.09375 to 0.09375
Outputs:
- outputs: bfloat16 [2, 12288, 1024], P(None, ('dp', 'tensor'))
- input_grad: bfloat16 [2, 12288, 1024], P(None, ('dp', 'tensor'))
- grad_gains: float32 [2, 2, 1024], P(None, None, 'dp')
- grad_shifts: float32 [2, 4, 1024], P(None, None, 'dp')
- grad_project_in: float32 [2, 1024, 16, 192], P(None, 'dp', 'tensor')
- grad_bias_in: float32 [2, 16, 128], P(None, 'tensor', 'dp')
- grad_project_out: float32 [2, 16, 64, 1024], P(None, 'tensor', None, 'dp')
- grad_up_weight: float32 [2, 1024, 4096], P(None, 'dp', 'tensor')
- grad_up_bias: float32 [2, 16, 256], P(None, 'tensor', 'dp')
- grad_down_weight: float32 [2, 4096, 1024], P(None, 'tensor', 'dp')
The draws below stay inside these ranges and needn't reach their ends.
All inputs are finite; a program needn't handle non-finite values.
Results may differ from the reference program's by a relative error of at most 0.023.
Values may be sent and summed in bfloat16 or wider, within the bound.
No kernel may reach another device: no remote copies, remote signals or barrier semaphores. Data moves between devices by JAX's collectives and lax.ppermute only.
A program may use at most 576 MiB of HBM per device.

```python
import jax
import jax.numpy as jnp
from jax import lax

D = 1024
HEADS = 16
HD = 64
FF = 4096
LAYERS = 2
MICRO = 2
SEQ = 384
ROWS_DEV = 384
ROWS = 12288
N_DP = 4
N_TENSOR = 8


def strengthened(values, stream_key, source, target, blocks, factor):
    owner, partner = [(jnp.arange(values.shape[dim]) // (values.shape[dim] // blocks)).reshape([-1 if axis == dim else 1 for axis in range(values.ndim)]) for dim in (source, target)]
    chosen = jax.random.permutation(stream_key, blocks)[partner]
    strong = (owner == chosen) | (owner == (partner + blocks // 2) % blocks)
    return jnp.where(strong, factor * values, values)


def block_scale(rng, shape, split, low, high):
    def one(axis_at, parts):
        steps = jax.random.uniform(jax.random.fold_in(jax.random.fold_in(rng, 6), axis_at), (parts,), jnp.float32, low / len(split), high / len(split))
        return jnp.repeat(jnp.exp(steps), shape[axis_at] // parts).reshape((-1,) + (1,) * (len(shape) - axis_at - 1))

    level = one(*split[0])
    for cut in split[1:]:
        level = level * one(*cut)
    return level


def noise(stream_key, shape, deviation, limit, pieces=(), held_as=jnp.bfloat16):
    loudness = block_scale(stream_key, shape, pieces, -0.22, 0.18) if pieces else 1.0
    entries = jax.random.normal(stream_key, shape, jnp.float32) * deviation * loudness
    return jnp.minimum(jnp.maximum(entries, -limit), limit).astype(held_as)


def bell_draw_with(rng, shape, deviation, reach, cuts, heavy, dtype=jnp.bfloat16):
    array = deviation * jax.random.normal(rng, shape, jnp.float32)
    if cuts:
        array = array * block_scale(rng, shape, cuts, -0.22, 0.18)
    return jnp.clip(strengthened(array, jax.random.fold_in(rng, 3), *heavy), -reach, reach).astype(dtype)


def setup_inputs(seed: int = 0) -> dict:
    keys = jax.random.split(jax.random.key(seed), 11)
    return {
        "inputs": bell_draw_with(keys[0], (MICRO, ROWS, D), 1.0, 6.0, ((1, 32),), (1, 2, 32, 2.75)),
        "cotangent": bell_draw_with(keys[1], (MICRO, ROWS, D), 1.0, 6.0, ((1, 32),), (1, 2, 32, 2.75)),
        "norm_gains": jnp.clip(1.0 + 0.1 * jax.random.normal(keys[2], (LAYERS, 2, D), jnp.float32), 0.5, 1.5).astype(jnp.bfloat16),
        "norm_shifts": noise(keys[3], (LAYERS, 4, D), 0.3, 2.5, ((2, 4),)),
        "project_in": noise(keys[4], (LAYERS, D, HEADS, 3 * HD), D ** -0.5, 0.1875, ((1, 4), (2, 8))),
        "bias_in": noise(keys[5], (LAYERS, HEADS, 2 * HD), 0.1, 1.5, ((1, 8), (2, 4))),
        "project_out": noise(keys[6], (LAYERS, HEADS, HD, D), (D // 16) ** -0.5, 0.75, ((1, 8), (3, 4))),
        "up_weight": noise(keys[7], (LAYERS, D, FF), D ** -0.5, 0.1875, ((1, 4), (2, 8))),
        "up_bias": noise(keys[8], (LAYERS, HEADS, FF // HEADS), 0.3, 2.5, ((1, 8), (2, 4))),
        "down_weight": noise(keys[9], (LAYERS, FF, D), FF ** -0.5, 0.09375, ((1, 8), (2, 4))),
    }


@jax.custom_vjp
def low(v):
    return lax.optimization_barrier(v.astype(jnp.bfloat16)).astype(jnp.float32)

@jax.custom_vjp
def low_back(v):
    return v

def low_keep(v):
    return (low(v), None)

def low_pass(kept, grad):
    return (grad,)

def back_keep(v):
    return (v, None)

def back_low(kept, grad):
    return (low(grad),)
low.defvjp(low_keep, low_pass)
low_back.defvjp(back_keep, back_low)
EPSILON = 1e-06
ROOT_HALF = 0.7071067811865476
EXACT = lax.Precision.HIGHEST

def layer_norm(values, gain, shift):
    centred = values - lax.optimization_barrier(jnp.mean(values, axis=-1, keepdims=True))
    spread = lax.optimization_barrier(jnp.mean(centred * centred, axis=-1, keepdims=True))
    return centred * lax.rsqrt(spread + EPSILON) * gain + shift

def gelu(values):
    return 0.5 * values * (1.0 + lax.erf(values * ROOT_HALF))

def attend_image(items):
    query, key, value = items
    scores = jnp.einsum('shd,thd->hst', query, key, precision=EXACT) * HD ** (-0.5)
    scores = low_back(scores)
    highest = lax.optimization_barrier(jnp.max(scores, axis=-1, keepdims=True))
    powers = jnp.exp(scores - highest)
    shares = powers / lax.optimization_barrier(jnp.sum(powers, axis=-1, keepdims=True))
    return jnp.einsum('hst,thd->shd', low(shares), value, precision=EXACT)

def encoder_layer(values, gains, shifts, project_in, bias_in, project_out, up_weight, up_bias, down_weight):
    count = values.shape[0]
    norm_one = low(layer_norm(values, gains[0], shifts[0]))
    projected = jnp.einsum('rd,dhc->rhc', norm_one, project_in, precision=EXACT)
    query = low_back(low(projected[:, :, :HD] + bias_in[:, :HD]))
    key = low_back(low(projected[:, :, HD:2 * HD]))
    value = low_back(low(projected[:, :, 2 * HD:] + bias_in[:, HD:]))
    shape = (count // SEQ, SEQ, HEADS, HD)
    mixed = lax.map(jax.checkpoint(attend_image), (query.reshape(shape), key.reshape(shape), value.reshape(shape)))
    mixed = low_back(low(mixed.reshape(count, HEADS, HD)))
    attended = low_back(jnp.einsum('rhd,hde->re', mixed, project_out, precision=EXACT) + shifts[2])
    hidden = values + attended
    norm_two = low(layer_norm(hidden, gains[1], shifts[1]))
    before = low_back(jnp.dot(norm_two, up_weight, precision=EXACT, preferred_element_type=jnp.float32) + up_bias.reshape(-1))
    active = low(gelu(before))
    branch = low_back(jnp.dot(active, down_weight, precision=EXACT, preferred_element_type=jnp.float32) + shifts[3])
    return hidden + branch

def forward(values, params):
    gains, shifts, project_in, bias_in, project_out, up_weight, up_bias, down_weight = params
    for layer in range(LAYERS):
        values = encoder_layer(values, gains[layer], shifts[layer], project_in[layer], bias_in[layer], project_out[layer], up_weight[layer], up_bias[layer], down_weight[layer])
    return values

def add_arrays(before, update):
    return before + update

def reference(inputs, cotangent, norm_gains, norm_shifts, project_in, bias_in, project_out, up_weight, up_bias, down_weight):
    params = tuple((piece.astype(jnp.float32) for piece in (norm_gains, norm_shifts, project_in, bias_in, project_out, up_weight, up_bias, down_weight)))
    group = ROWS_DEV * N_TENSOR
    blocks = MICRO * N_DP
    values = inputs.astype(jnp.float32).reshape(blocks, group, D)
    grads = cotangent.astype(jnp.float32).reshape(blocks, group, D)

    def step(totals, pair):
        block_rows, block_grad = pair
        result, pull = jax.vjp(forward, block_rows, params)
        grad_rows, grad_params = pull(block_grad)
        totals = jax.tree.map(add_arrays, totals, grad_params)
        return (totals, (result.astype(jnp.bfloat16), grad_rows.astype(jnp.bfloat16)))
    zeros = jax.tree.map(jnp.zeros_like, params)
    totals, (results, backs) = lax.scan(step, zeros, (values, grads))
    return (results.reshape(MICRO, ROWS, D), backs.reshape(MICRO, ROWS, D), totals[0], totals[1], totals[2], totals[3], totals[4], totals[5], totals[6], totals[7])
```

```python
import functools
import itertools

import jax
import jax.numpy as jnp
from jax import lax
from jax.experimental import pallas as pl
from jax.experimental.pallas import tpu as pltpu
from jax.sharding import PartitionSpec as P

SEQ = 384
EPSILON = 1e-06
ROOT_HALF = 0.7071067811865476
ROOT_TWO_PI_INVERSE = 0.3989422804014327
NARROW = jnp.bfloat16
SINGLE = jnp.float32


def dot(left, right, dims):
    return lax.dot_general(left, right, (dims, ((), ())), preferred_element_type=SINGLE)


def plain(left, right):
    return dot(left, right, ((1,), (0,)))


def by_rows(left, right):
    return dot(left, right, ((0,), (0,)))


def by_columns(left, right):
    return dot(left, right, ((1,), (1,)))


def swap(values, axis, bit):
    size = lax.axis_size(axis)
    return lax.ppermute(values, axis, [(i, i ^ (1 << bit)) for i in range(size)])


def bits_of(axis):
    size = lax.axis_size(axis)
    count = size.bit_length() - 1
    assert size == 1 << count
    return count


def hop_order(color):
    far = list(range(bits_of("tensor") - 1, 0, -1))
    wide = list(range(bits_of("dp")))
    if color:
        wide.reverse()
    order = []
    for one, two in itertools.zip_longest(far, wide):
        if one is not None:
            order.append(("tensor", one))
        if two is not None:
            order.append(("dp", two))
    return order + [("tensor", 0)]


def pieces_of(values, axis, inner):
    return [
        lax.slice_in_dim(values, at, at + inner, axis=axis) for at in range(0, values.shape[axis], inner)
    ]


def interleave(mine, theirs, axis, inner):
    if inner == mine.shape[axis]:
        return jnp.concatenate([mine, theirs], axis=axis)
    both = zip(pieces_of(mine, axis, inner), pieces_of(theirs, axis, inner), strict=True)
    return jnp.concatenate([piece for pair in both for piece in pair], axis=axis)


def part(values, axis, inner, which):
    runs = pieces_of(values, axis, inner)[which::2]
    return runs[0] if len(runs) == 1 else jnp.concatenate(runs, axis=axis)


def places(order, feature_axis, block):
    found = []
    present = []
    for name, bit in order:
        if name == "dp":
            lower = sum(1 for other in present if other < bit)
            found.append((feature_axis, block << lower))
            present.append(bit)
        else:
            found.append((1 - feature_axis, None))
    return found


def gather(shard, color, feature_axis):
    order = hop_order(color)
    held = shard
    for (name, bit), (axis, inner) in zip(
        order[:-1], places(order[:-1], feature_axis, shard.shape[feature_axis]), strict=True
    ):
        theirs = swap(held, name, bit)
        held = interleave(held, theirs, axis, held.shape[axis] if inner is None else inner)
    name, bit = order[-1]
    return held, swap(held, name, bit)


def add(left, right):
    return left.astype(SINGLE) + right.astype(SINGLE)


def scatter(own, other, color, feature_axis, block):
    order = hop_order(color)
    name, bit = order[-1]
    total = add(own, swap(other, name, bit))
    spots = places(order[:-1], feature_axis, block)
    for (name, bit), (axis, inner) in reversed(list(zip(order[:-1], spots, strict=True))):
        total = total.astype(NARROW)
        inner = total.shape[axis] // 2 if inner is None else inner
        theirs = swap(part(total, axis, inner, 1), name, bit)
        total = add(part(total, axis, inner, 0), theirs)
    return total


def flipped(values, axis, name):
    count = bits_of(name)
    me = lax.axis_index(name)
    block = values.shape[axis] >> count
    for bit in range(count):
        run = block << bit
        runs = pieces_of(values, axis, run)
        turned = jnp.concatenate([runs[at ^ 1] for at in range(len(runs))], axis=axis)
        values = jnp.where((me >> bit) & 1 == 1, turned, values)
    return values


def unit_order(blocks, name="tensor"):
    count = bits_of(name)
    rest = blocks.shape[1:]
    split = blocks.reshape((2,) * count + rest)
    turned = split.transpose(tuple(reversed(range(count))) + tuple(range(count, split.ndim)))
    return turned.reshape(blocks.shape)


def normal(values):
    centred = values - jnp.mean(values, axis=-1, keepdims=True)
    spread = jnp.mean(centred * centred, axis=-1, keepdims=True)
    scale = lax.rsqrt(spread + EPSILON)
    return centred * scale, scale


def normal_back(hat, scale, gain, grad):
    scaled = grad * gain
    return scale * (
        scaled
        - jnp.mean(scaled, axis=-1, keepdims=True)
        - hat * jnp.mean(scaled * hat, axis=-1, keepdims=True)
    )


def attend_kernel(heads, size, scale, packed_ref, mixed_ref, shares_ref):
    for head in range(heads):
        at = head * 3 * size
        query = (packed_ref[:, at : at + size].astype(SINGLE) * scale).astype(NARROW)
        key = packed_ref[:, at + size : at + 2 * size]
        value = packed_ref[:, at + 2 * size : at + 3 * size]
        scores = by_columns(query, key)
        powers = jnp.exp(scores - jnp.max(scores, axis=-1, keepdims=True))
        shares = (powers * (1.0 / jnp.sum(powers, axis=-1, keepdims=True))).astype(NARROW)
        shares_ref[0, head] = shares
        mixed_ref[:, head * size : (head + 1) * size] = plain(shares, value).astype(NARROW)


def attend_back_kernel(heads, size, scale, packed_ref, shares_ref, grad_ref, out_ref, sums_ref):
    for head in range(heads):
        at = head * 3 * size
        query = packed_ref[:, at : at + size]
        key = packed_ref[:, at + size : at + 2 * size]
        value = packed_ref[:, at + 2 * size : at + 3 * size]
        grad = grad_ref[:, head * size : (head + 1) * size]
        narrow_shares = shares_ref[0, head]
        shares = narrow_shares.astype(SINGLE)
        grad_shares = by_columns(grad, value)
        weighted = jnp.sum(shares * grad_shares, axis=-1, keepdims=True)
        grad_scores = (shares * (grad_shares - weighted)).astype(NARROW)
        grad_query = (plain(grad_scores, key) * scale).astype(NARROW)
        grad_key = (by_rows(query, grad_scores) * scale).T.astype(NARROW)
        grad_value = by_rows(grad, narrow_shares).T.astype(NARROW)
        out_ref[:, at : at + size] = grad_query
        out_ref[:, at + size : at + 2 * size] = grad_key
        out_ref[:, at + 2 * size : at + 3 * size] = grad_value
    sums_ref[0, 0] = jnp.sum(out_ref[...].astype(SINGLE), axis=0, keepdims=True)


def attend_forward(packed, group, size, scale):
    images = packed.shape[0] // SEQ
    heads = packed.shape[1] // (3 * size)
    return pl.pallas_call(
        functools.partial(attend_kernel, group, size, scale),
        grid=(images, heads // group),
        in_specs=[pl.BlockSpec((SEQ, group * 3 * size), lambda i, g: (i, g))],
        out_specs=[
            pl.BlockSpec((SEQ, group * size), lambda i, g: (i, g)),
            pl.BlockSpec((1, group, SEQ, SEQ), lambda i, g: (i, g, 0, 0)),
        ],
        out_shape=[
            jax.ShapeDtypeStruct((packed.shape[0], heads * size), NARROW),
            jax.ShapeDtypeStruct((images, heads, SEQ, SEQ), NARROW),
        ],
        cost_estimate=pl.CostEstimate(
            flops=4 * images * heads * SEQ * SEQ * size,
            bytes_accessed=2 * packed.size + 2 * images * heads * SEQ * SEQ,
            transcendentals=images * heads * SEQ * SEQ,
        ),
        name="attend_forward",
    )(packed)


def attend_backward(packed, shares, grad, group, size, scale):
    images = packed.shape[0] // SEQ
    heads = packed.shape[1] // (3 * size)
    return pl.pallas_call(
        functools.partial(attend_back_kernel, group, size, scale),
        grid=(images, heads // group),
        in_specs=[
            pl.BlockSpec((SEQ, group * 3 * size), lambda i, g: (i, g)),
            pl.BlockSpec((1, group, SEQ, SEQ), lambda i, g: (i, g, 0, 0)),
            pl.BlockSpec((SEQ, group * size), lambda i, g: (i, g)),
        ],
        out_specs=[
            pl.BlockSpec((SEQ, group * 3 * size), lambda i, g: (i, g)),
            pl.BlockSpec((1, 1, 1, group * 3 * size), lambda i, g: (i, g, 0, 0)),
        ],
        out_shape=[
            jax.ShapeDtypeStruct(packed.shape, NARROW),
            jax.ShapeDtypeStruct((images, heads // group, 1, group * 3 * size), SINGLE),
        ],
        cost_estimate=pl.CostEstimate(
            flops=10 * images * heads * SEQ * SEQ * size,
            bytes_accessed=6 * packed.size + 2 * images * heads * SEQ * SEQ,
            transcendentals=0,
        ),
        name="attend_backward",
    )(packed, shares, grad)


def layer_forward(values, small, weights, size):
    gains, shifts, bias_in, bias_up = small
    enter, leave, up, down = weights
    scale = size ** (-0.5)
    hat_one, scale_one = normal(values)
    norm_one = (hat_one * gains[0] + shifts[0]).astype(NARROW)
    packed = [(plain(norm_one, enter[c]) + bias_in[c]).astype(NARROW) for c in range(2)]
    attended = [attend_forward(packed[c], group_of(packed[c], size), size, scale) for c in range(2)]
    mixed = [attended[c][0] for c in range(2)]
    shares = [attended[c][1] for c in range(2)]
    hidden = values + (plain(mixed[0], leave[0]) + plain(mixed[1], leave[1])) + shifts[2]
    hat_two, scale_two = normal(hidden)
    norm_two = (hat_two * gains[1] + shifts[1]).astype(NARROW)
    active = []
    slopes = []
    for c in range(2):
        before = plain(norm_two, up[c]) + bias_up[c]
        curve = 0.5 * (1.0 + lax.erf(before * ROOT_HALF))
        active.append((before * curve).astype(NARROW))
        slopes.append(
            (curve + before * jnp.exp(-0.5 * before * before) * ROOT_TWO_PI_INVERSE).astype(NARROW)
        )
    result = hidden + (plain(active[0], down[0]) + plain(active[1], down[1])) + shifts[3]
    return result, (values, norm_one, packed, shares, mixed, hidden, norm_two, active, slopes)


def group_of(packed, size):
    heads = packed.shape[1] // (3 * size)
    return 2 if heads % 2 == 0 else 1


def layer_backward(grad_out, kept, small, weights, size):
    gains, shifts, bias_in, bias_up = small
    enter, leave, up, down = weights
    values, norm_one, packed, shares, mixed, hidden, norm_two, active, slopes = kept
    scale = size ** (-0.5)
    branch = grad_out.astype(NARROW)
    shift_down = jnp.sum(branch.astype(SINGLE), axis=0)
    before = [(by_columns(branch, down[c]) * slopes[c].astype(SINGLE)).astype(NARROW) for c in range(2)]
    grad_down = [by_rows(active[c], branch).astype(NARROW) for c in range(2)]
    grad_up = [by_rows(norm_two, before[c]).astype(NARROW) for c in range(2)]
    bias_up_grad = [jnp.sum(before[c].astype(SINGLE), axis=0) for c in range(2)]
    grad_norm = by_columns(before[0], up[0]) + by_columns(before[1], up[1])
    hat, spread = normal(hidden)
    gain_two = jnp.sum(grad_norm * hat, axis=0)
    shift_two = jnp.sum(grad_norm, axis=0)
    grad_hidden = grad_out + normal_back(hat, spread, gains[1], grad_norm)
    heads_grad = grad_hidden.astype(NARROW)
    shift_out = jnp.sum(heads_grad.astype(SINGLE), axis=0)
    grad_mixed = [by_columns(heads_grad, leave[c]).astype(NARROW) for c in range(2)]
    grad_leave = [by_rows(mixed[c], heads_grad).astype(NARROW) for c in range(2)]
    both = [
        attend_backward(packed[c], shares[c], grad_mixed[c], group_of(packed[c], size), size, scale)
        for c in range(2)
    ]
    grad_packed = [both[c][0] for c in range(2)]
    bias_in_grad = [jnp.sum(both[c][1], axis=(0, 2)).reshape(-1, 3 * size) for c in range(2)]
    grad_enter = [by_rows(norm_one, grad_packed[c]).astype(NARROW) for c in range(2)]
    grad_first = by_columns(grad_packed[0], enter[0]) + by_columns(grad_packed[1], enter[1])
    hat_one, spread_one = normal(values)
    gain_one = jnp.sum(grad_first * hat_one, axis=0)
    shift_one = jnp.sum(grad_first, axis=0)
    grad_inputs = grad_hidden + normal_back(hat_one, spread_one, gains[0], grad_first)
    return (
        grad_inputs,
        (grad_enter, grad_leave, grad_up, grad_down),
        (
            jnp.stack([gain_one, gain_two]),
            jnp.stack([shift_one, shift_two, shift_out, shift_down]),
            jnp.concatenate(bias_in_grad, axis=0),
            jnp.concatenate(bias_up_grad, axis=0),
        ),
    )


FEATURES = (0, 1, 0, 1)
COLORS = ((0, 1, 1, 0), (1, 0, 0, 1))


def gather_small(norm_gains, norm_shifts, bias_in, up_bias, size):
    layers = norm_gains.shape[0]
    across, deep = lax.axis_size("dp"), lax.axis_size("tensor")
    flat = jnp.concatenate([v.reshape(-1) for v in (norm_gains, norm_shifts, bias_in, up_bias)])
    full = lax.all_gather(flat, ("dp", "tensor"), axis=0).reshape(across, deep, -1)
    ends = list(itertools.accumulate(v.size for v in (norm_gains, norm_shifts, bias_in, up_bias)))
    gains, shifts, enter, up = jnp.split(full, ends[:-1], axis=2)

    def features(piece, rows):
        piece = piece[:, 0].reshape(across, layers, rows, -1).transpose(1, 2, 0, 3)
        return flipped(piece.reshape(layers, rows, -1), 2, "dp").astype(SINGLE)

    def units(piece, rows):
        piece = piece.reshape(across, deep, layers, rows, -1).transpose(1, 2, 3, 0, 4)
        return unit_order(flipped(piece, 0, "tensor")).astype(SINGLE)

    gains = features(gains, norm_gains.shape[1])
    shifts = features(shifts, norm_shifts.shape[1])
    enter = units(enter, bias_in.shape[1])
    up = units(up, up_bias.shape[1])
    enter = enter.transpose(1, 0, 2, 3, 4).reshape(layers, 2, -1, 2 * size)
    zero = jnp.zeros_like(enter[..., :size])
    enter = jnp.concatenate([enter[..., :size], zero, enter[..., size:]], axis=-1)
    enter = enter.reshape(layers, 2, -1)
    up = up.transpose(1, 0, 2, 3, 4).reshape(layers, 2, -1)
    return [(gains[l], shifts[l], enter[l], up[l]) for l in range(layers)]


def sum_small(parts, shapes, size):
    layers = len(parts)
    across, deep = lax.axis_size("dp"), lax.axis_size("tensor")
    gains = jnp.stack([p[0] for p in parts])
    shifts = jnp.stack([p[1] for p in parts])
    gains = flipped(gains, 2, "dp")
    shifts = flipped(shifts, 2, "dp")

    def units(values):
        blocks = values.reshape(layers, deep, -1).transpose(1, 0, 2)
        return flipped(unit_order(blocks), 0, "tensor")

    enter = jnp.stack([p[2] for p in parts])
    enter = jnp.concatenate([enter[..., :size], enter[..., 2 * size :]], axis=-1)
    enter = units(enter)
    up = units(jnp.stack([p[3] for p in parts]))
    flat = jnp.concatenate([v.reshape(-1) for v in (gains, shifts, enter, up)])
    total = lax.psum(flat, ("dp", "tensor"))
    ends = list(itertools.accumulate(v.size for v in (gains, shifts, enter, up)))
    gains_t, shifts_t, enter_t, up_t = jnp.split(total, ends[:-1])
    row, column = lax.axis_index("dp"), lax.axis_index("tensor")

    def mine(values, axis, index, count):
        width = values.shape[axis] // count
        return lax.dynamic_slice_in_dim(values, index * width, width, axis=axis)

    gains_t = mine(gains_t.reshape(gains.shape), 2, row, across)
    shifts_t = mine(shifts_t.reshape(shifts.shape), 2, row, across)
    enter_t = mine(enter_t.reshape(enter.shape), 0, column, deep)
    enter_t = mine(enter_t.reshape(shapes[0][:2] + (-1,)), 2, row, across)
    up_t = mine(up_t.reshape(up.shape), 0, column, deep)
    up_t = mine(up_t.reshape(shapes[1][:2] + (-1,)), 2, row, across)
    return gains_t, shifts_t, enter_t, up_t


def shards(
    inputs,
    cotangent,
    norm_gains,
    norm_shifts,
    project_in,
    bias_in,
    project_out,
    up_weight,
    up_bias,
    down_weight,
):
    layers = project_in.shape[0]
    width = inputs.shape[2]
    size = project_out.shape[2]
    shapes = inputs.shape
    small = gather_small(norm_gains, norm_shifts, bias_in, up_bias, size)
    flat = [
        (
            project_in[l].reshape(project_in.shape[1], -1),
            project_out[l].reshape(-1, project_out.shape[3]),
            up_weight[l],
            down_weight[l],
        )
        for l in range(layers)
    ]
    weights = [
        [gather(flat[l][k], COLORS[l % 2][k], FEATURES[k]) for k in range(4)] for l in range(layers)
    ]
    values = flipped(inputs.reshape(-1, width), 1, "dp").astype(SINGLE)
    kept = []
    for l in range(layers):
        values, saved = layer_forward(values, small[l], weights[l], size)
        kept.append(saved)
    outputs = flipped(values.astype(NARROW), 1, "dp").reshape(shapes)
    grad = flipped(cotangent.reshape(-1, width), 1, "dp").astype(SINGLE)
    owned = [None] * layers
    parts = [None] * layers
    for l in reversed(range(layers)):
        grad, big, parts[l] = layer_backward(grad, kept[l], small[l], weights[l], size)
        owned[l] = [
            scatter(big[k][0], big[k][1], COLORS[l % 2][k], FEATURES[k], flat[l][k].shape[FEATURES[k]])
            for k in range(4)
        ]
    input_grad = flipped(grad.astype(NARROW), 1, "dp").reshape(shapes)
    gains, shifts, enter_bias, up_bias_grad = sum_small(parts, (bias_in.shape, up_bias.shape), size)
    stacked = [jnp.stack([owned[l][k] for l in range(layers)]) for k in range(4)]
    return (
        outputs,
        input_grad,
        gains,
        shifts,
        stacked[0].reshape(project_in.shape),
        enter_bias,
        stacked[1].reshape(project_out.shape),
        stacked[2],
        up_bias_grad,
        stacked[3],
    )


def solution(mesh):
    specs = (
        P(None, ("dp", "tensor"), None),
        P(None, ("dp", "tensor"), None),
        P(None, None, "dp"),
        P(None, None, "dp"),
        P(None, "dp", "tensor", None),
        P(None, "tensor", "dp"),
        P(None, "tensor", None, "dp"),
        P(None, "dp", "tensor"),
        P(None, "tensor", "dp"),
        P(None, "tensor", "dp"),
    )
    return jax.shard_map(shards, mesh=mesh, in_specs=specs, out_specs=specs, check_vma=False)
```

```python
import functools
import itertools

import jax
import jax.numpy as jnp
from jax import lax
from jax.experimental import pallas as pl
from jax.sharding import PartitionSpec as P

SEQ = 384
EPSILON = 1e-06
ROOT_HALF = 0.7071067811865476
ROOT_TWO_PI_INVERSE = 0.3989422804014327
NARROW = jnp.bfloat16
SINGLE = jnp.float32


def dot(left, right, dims):
    return lax.dot_general(left, right, (dims, ((), ())), preferred_element_type=SINGLE)


def plain(left, right):
    return dot(left, right, ((1,), (0,)))


def by_rows(left, right):
    return dot(left, right, ((0,), (0,)))


def by_columns(left, right):
    return dot(left, right, ((1,), (1,)))


def swap(values, axis, bit):
    size = lax.axis_size(axis)
    return lax.ppermute(values, axis, [(i, i ^ (1 << bit)) for i in range(size)])


def bits_of(axis):
    size = lax.axis_size(axis)
    count = size.bit_length() - 1
    assert size == 1 << count
    return count


def hop_order(color):
    far = list(range(bits_of("tensor") - 1, 0, -1))
    wide = list(range(bits_of("dp")))
    if color:
        wide.reverse()
    order = []
    for one, two in itertools.zip_longest(far, wide):
        if one is not None:
            order.append(("tensor", one))
        if two is not None:
            order.append(("dp", two))
    return order + [("tensor", 0)]


def pieces_of(values, axis, inner):
    return [
        lax.slice_in_dim(values, at, at + inner, axis=axis) for at in range(0, values.shape[axis], inner)
    ]


def interleave(mine, theirs, axis, inner):
    if inner == mine.shape[axis]:
        return jnp.concatenate([mine, theirs], axis=axis)
    both = zip(pieces_of(mine, axis, inner), pieces_of(theirs, axis, inner), strict=True)
    return jnp.concatenate([piece for pair in both for piece in pair], axis=axis)


def part(values, axis, inner, which):
    runs = pieces_of(values, axis, inner)[which::2]
    return runs[0] if len(runs) == 1 else jnp.concatenate(runs, axis=axis)


def places(order, feature_axis, block):
    found = []
    present = []
    for name, bit in order:
        if name == "dp":
            lower = sum(1 for other in present if other < bit)
            found.append((feature_axis, block << lower))
            present.append(bit)
        else:
            found.append((1 - feature_axis, None))
    return found


def gather(shard, color, feature_axis):
    order = hop_order(color)
    held = shard
    spots = places(order[:-1], feature_axis, shard.shape[feature_axis])
    for (name, bit), (axis, inner) in zip(order[:-1], spots, strict=True):
        theirs = swap(held, name, bit)
        held = interleave(held, theirs, axis, held.shape[axis] if inner is None else inner)
    name, bit = order[-1]
    return held, swap(held, name, bit)


def add(left, right):
    return left.astype(SINGLE) + right.astype(SINGLE)


def scatter(own, other, color, feature_axis, block):
    order = hop_order(color)
    name, bit = order[-1]
    total = add(own, swap(other.astype(NARROW), name, bit))
    spots = places(order[:-1], feature_axis, block)
    back = reversed(list(zip(order[:-1], spots, strict=True)))
    for (name, bit), (axis, inner) in back:
        total = total.astype(NARROW)
        inner = total.shape[axis] // 2 if inner is None else inner
        theirs = swap(part(total, axis, inner, 1), name, bit)
        total = add(part(total, axis, inner, 0), theirs)
    return total


def flipped(values, axis, name):
    count = bits_of(name)
    me = lax.axis_index(name)
    block = values.shape[axis] >> count
    for bit in range(count):
        run = block << bit
        runs = pieces_of(values, axis, run)
        turned = jnp.concatenate([runs[at ^ 1] for at in range(len(runs))], axis=axis)
        values = jnp.where((me >> bit) & 1 == 1, turned, values)
    return values


def unit_order(blocks, name="tensor"):
    count = bits_of(name)
    rest = blocks.shape[1:]
    split = blocks.reshape((2,) * count + rest)
    turned = split.transpose(tuple(reversed(range(count))) + tuple(range(count, split.ndim)))
    return turned.reshape(blocks.shape)


def normal(values):
    centred = values - jnp.mean(values, axis=-1, keepdims=True)
    spread = jnp.mean(centred * centred, axis=-1, keepdims=True)
    scale = lax.rsqrt(spread + EPSILON)
    return centred * scale, scale


def normal_back(hat, scale, gain, grad):
    scaled = grad * gain
    return scale * (
        scaled
        - jnp.mean(scaled, axis=-1, keepdims=True)
        - hat * jnp.mean(scaled * hat, axis=-1, keepdims=True)
    )


def attend_kernel(heads, size, scale, packed_ref, mixed_ref, shares_ref):
    for head in range(heads):
        at = head * 3 * size
        query = (packed_ref[:, at : at + size].astype(SINGLE) * scale).astype(NARROW)
        key = packed_ref[:, at + size : at + 2 * size]
        value = packed_ref[:, at + 2 * size : at + 3 * size]
        scores = by_columns(query, key)
        powers = jnp.exp(scores - jnp.max(scores, axis=-1, keepdims=True))
        shares = (powers * (1.0 / jnp.sum(powers, axis=-1, keepdims=True))).astype(NARROW)
        shares_ref[0, head] = shares
        mixed_ref[:, head * size : (head + 1) * size] = plain(shares, value).astype(NARROW)


def attend_back_kernel(heads, size, scale, packed_ref, shares_ref, grad_ref, out_ref, sums_ref):
    for head in range(heads):
        at = head * 3 * size
        query = packed_ref[:, at : at + size]
        key = packed_ref[:, at + size : at + 2 * size]
        value = packed_ref[:, at + 2 * size : at + 3 * size]
        grad = grad_ref[:, head * size : (head + 1) * size]
        narrow_shares = shares_ref[0, head]
        shares = narrow_shares.astype(SINGLE)
        grad_shares = by_columns(grad, value)
        weighted = jnp.sum(shares * grad_shares, axis=-1, keepdims=True)
        grad_scores = (shares * (grad_shares - weighted)).astype(NARROW)
        grad_query = (plain(grad_scores, key) * scale).astype(NARROW)
        grad_key = (by_rows(query, grad_scores) * scale).T.astype(NARROW)
        grad_value = by_rows(grad, narrow_shares).T.astype(NARROW)
        out_ref[:, at : at + size] = grad_query
        out_ref[:, at + size : at + 2 * size] = grad_key
        out_ref[:, at + 2 * size : at + 3 * size] = grad_value
    sums_ref[0, 0] = jnp.sum(out_ref[...].astype(SINGLE), axis=0, keepdims=True)


def attend_forward(packed, group, size, scale):
    images = packed.shape[0] // SEQ
    heads = packed.shape[1] // (3 * size)
    return pl.pallas_call(
        functools.partial(attend_kernel, group, size, scale),
        grid=(images, heads // group),
        in_specs=[pl.BlockSpec((SEQ, group * 3 * size), lambda i, g: (i, g))],
        out_specs=[
            pl.BlockSpec((SEQ, group * size), lambda i, g: (i, g)),
            pl.BlockSpec((1, group, SEQ, SEQ), lambda i, g: (i, g, 0, 0)),
        ],
        out_shape=[
            jax.ShapeDtypeStruct((packed.shape[0], heads * size), NARROW),
            jax.ShapeDtypeStruct((images, heads, SEQ, SEQ), NARROW),
        ],
        cost_estimate=pl.CostEstimate(
            flops=4 * images * heads * SEQ * SEQ * size,
            bytes_accessed=2 * packed.size + 2 * images * heads * SEQ * SEQ,
            transcendentals=images * heads * SEQ * SEQ,
        ),
        name="attend_forward",
    )(packed)


def attend_backward(packed, shares, grad, group, size, scale):
    images = packed.shape[0] // SEQ
    heads = packed.shape[1] // (3 * size)
    return pl.pallas_call(
        functools.partial(attend_back_kernel, group, size, scale),
        grid=(images, heads // group),
        in_specs=[
            pl.BlockSpec((SEQ, group * 3 * size), lambda i, g: (i, g)),
            pl.BlockSpec((1, group, SEQ, SEQ), lambda i, g: (i, g, 0, 0)),
            pl.BlockSpec((SEQ, group * size), lambda i, g: (i, g)),
        ],
        out_specs=[
            pl.BlockSpec((SEQ, group * 3 * size), lambda i, g: (i, g)),
            pl.BlockSpec((1, 1, 1, group * 3 * size), lambda i, g: (i, g, 0, 0)),
        ],
        out_shape=[
            jax.ShapeDtypeStruct(packed.shape, NARROW),
            jax.ShapeDtypeStruct((images, heads // group, 1, group * 3 * size), SINGLE),
        ],
        cost_estimate=pl.CostEstimate(
            flops=10 * images * heads * SEQ * SEQ * size,
            bytes_accessed=6 * packed.size + 2 * images * heads * SEQ * SEQ,
            transcendentals=0,
        ),
        name="attend_backward",
    )(packed, shares, grad)


def layer_forward(values, small, weights, size):
    gains, shifts, bias_in, bias_up = small
    enter, leave, up, down = weights
    scale = size ** (-0.5)
    hat_one, _ = normal(values)
    norm_one = (hat_one * gains[0] + shifts[0]).astype(NARROW)
    packed = [(plain(norm_one, enter[c]) + bias_in[c]).astype(NARROW) for c in range(2)]
    attended = []
    for c in range(2):
        attended.append(attend_forward(packed[c], group_of(packed[c], size), size, scale))
    mixed = [attended[c][0] for c in range(2)]
    shares = [attended[c][1] for c in range(2)]
    hidden = values + (plain(mixed[0], leave[0]) + plain(mixed[1], leave[1])) + shifts[2]
    hat_two, _ = normal(hidden)
    norm_two = (hat_two * gains[1] + shifts[1]).astype(NARROW)
    active = []
    slopes = []
    for c in range(2):
        before = plain(norm_two, up[c]) + bias_up[c]
        curve = 0.5 * (1.0 + lax.erf(before * ROOT_HALF))
        active.append((before * curve).astype(NARROW))
        slopes.append(
            (curve + before * jnp.exp(-0.5 * before * before) * ROOT_TWO_PI_INVERSE).astype(NARROW)
        )
    result = hidden + (plain(active[0], down[0]) + plain(active[1], down[1])) + shifts[3]
    return result, (values, norm_one, packed, shares, mixed, hidden, norm_two, active, slopes)


def group_of(packed, size):
    heads = packed.shape[1] // (3 * size)
    return 2 if heads % 2 == 0 else 1


def layer_backward(grad_out, kept, small, weights, size):
    gains, _, _, _ = small
    enter, leave, up, down = weights
    values, norm_one, packed, shares, mixed, hidden, norm_two, active, slopes = kept
    scale = size ** (-0.5)
    branch = grad_out.astype(NARROW)
    shift_down = jnp.sum(branch.astype(SINGLE), axis=0)
    before = [
        (by_columns(branch, down[c]) * slopes[c].astype(SINGLE)).astype(NARROW)
        for c in range(2)
    ]
    grad_down = [by_rows(active[c], branch) for c in range(2)]
    grad_up = [by_rows(norm_two, before[c]) for c in range(2)]
    bias_up_grad = [jnp.sum(before[c].astype(SINGLE), axis=0) for c in range(2)]
    grad_norm = by_columns(before[0], up[0]) + by_columns(before[1], up[1])
    hat, spread = normal(hidden)
    gain_two = jnp.sum(grad_norm * hat, axis=0)
    shift_two = jnp.sum(grad_norm, axis=0)
    grad_hidden = grad_out + normal_back(hat, spread, gains[1], grad_norm)
    heads_grad = grad_hidden.astype(NARROW)
    shift_out = jnp.sum(heads_grad.astype(SINGLE), axis=0)
    grad_mixed = [by_columns(heads_grad, leave[c]).astype(NARROW) for c in range(2)]
    grad_leave = [by_rows(mixed[c], heads_grad) for c in range(2)]
    both = []
    for c in range(2):
        both.append(
            attend_backward(
                packed[c], shares[c], grad_mixed[c], group_of(packed[c], size), size, scale
            )
        )
    grad_packed = [both[c][0] for c in range(2)]
    bias_in_grad = [jnp.sum(both[c][1], axis=(0, 2)).reshape(-1, 3 * size) for c in range(2)]
    grad_enter = [by_rows(norm_one, grad_packed[c]) for c in range(2)]
    grad_first = by_columns(grad_packed[0], enter[0]) + by_columns(grad_packed[1], enter[1])
    hat_one, spread_one = normal(values)
    gain_one = jnp.sum(grad_first * hat_one, axis=0)
    shift_one = jnp.sum(grad_first, axis=0)
    grad_inputs = grad_hidden + normal_back(hat_one, spread_one, gains[0], grad_first)
    return (
        grad_inputs,
        (grad_enter, grad_leave, grad_up, grad_down),
        (
            jnp.stack([gain_one, gain_two]),
            jnp.stack([shift_one, shift_two, shift_out, shift_down]),
            jnp.concatenate(bias_in_grad, axis=0),
            jnp.concatenate(bias_up_grad, axis=0),
        ),
    )


FEATURES = (0, 1, 0, 1)
COLORS = ((0, 1, 1, 0), (1, 0, 0, 1))


def gather_small(norm_gains, norm_shifts, bias_in, up_bias, size):
    layers = norm_gains.shape[0]
    across, deep = lax.axis_size("dp"), lax.axis_size("tensor")
    full = jnp.concatenate([v.reshape(-1) for v in (norm_gains, norm_shifts, bias_in, up_bias)])
    hops = [("dp", bit) for bit in range(bits_of("dp"))]
    hops += [("tensor", bit) for bit in range(bits_of("tensor"))]
    for name, bit in hops:
        full = jnp.concatenate([full, swap(full, name, bit)])
    full = full.reshape(deep, across, -1)
    ends = list(itertools.accumulate(v.size for v in (norm_gains, norm_shifts, bias_in, up_bias)))
    gains, shifts, enter, up = jnp.split(full, ends[:-1], axis=2)

    def features(piece, rows):
        piece = piece[0].reshape(across, layers, rows, -1).transpose(1, 2, 0, 3)
        return piece.reshape(layers, rows, -1).astype(SINGLE)

    def units(piece, rows):
        piece = flipped(piece.reshape(deep, across, layers, rows, -1), 1, "dp")
        return unit_order(piece.transpose(0, 2, 3, 1, 4)).astype(SINGLE)

    gains = features(gains, norm_gains.shape[1])
    shifts = features(shifts, norm_shifts.shape[1])
    enter = units(enter, bias_in.shape[1])
    up = units(up, up_bias.shape[1])
    enter = enter.transpose(1, 0, 2, 3, 4).reshape(layers, 2, -1, 2 * size)
    zero = jnp.zeros_like(enter[..., :size])
    enter = jnp.concatenate([enter[..., :size], zero, enter[..., size:]], axis=-1)
    enter = enter.reshape(layers, 2, -1)
    up = up.transpose(1, 0, 2, 3, 4).reshape(layers, 2, -1)
    return [(gains[l], shifts[l], enter[l], up[l]) for l in range(layers)]


def sum_small(grads, shapes, size):
    gains, shifts, enter, up = grads
    across, deep = lax.axis_size("dp"), lax.axis_size("tensor")
    features = jnp.concatenate([gains, shifts], axis=0)
    rows = features.shape[0]
    enter = jnp.concatenate([enter[:, :size], enter[:, 2 * size :]], axis=-1)

    def units(values, shape):
        blocks = flipped(values.reshape(deep, shape[1], across, shape[2]), 2, "dp")
        return unit_order(blocks).transpose(0, 2, 1, 3).reshape(deep, across, -1)

    both = jnp.concatenate([units(enter, shapes[0]), units(up, shapes[1])], axis=2)
    for bit in reversed(range(bits_of("tensor"))):
        half = both.shape[0] // 2
        sent = jnp.concatenate([features.reshape(-1), both[half:].reshape(-1)])
        got = swap(sent, "tensor", bit)
        features = features + got[: features.size].reshape(features.shape)
        both = both[:half] + got[features.size :].reshape(both[:half].shape)
    features = features.reshape(rows, across, -1).transpose(1, 0, 2).reshape(across, -1)
    total = jnp.concatenate([features, both[0]], axis=1)
    for bit in reversed(range(bits_of("dp"))):
        half = total.shape[0] // 2
        total = total[:half] + swap(total[half:], "dp", bit)
    features, enter, up = jnp.split(
        total[0], [features.shape[1], features.shape[1] + shapes[0][1] * shapes[0][2]]
    )
    features = features.reshape(rows, -1)
    return (
        features[: gains.shape[0]],
        features[gains.shape[0] :],
        enter.reshape(shapes[0][1:]),
        up.reshape(shapes[1][1:]),
    )


def step(
    inputs,
    cotangent,
    norm_gains,
    norm_shifts,
    project_in,
    bias_in,
    project_out,
    up_weight,
    up_bias,
    down_weight,
):
    layers = project_in.shape[0]
    width = inputs.shape[2]
    size = project_out.shape[2]
    shapes = inputs.shape
    small = gather_small(norm_gains, norm_shifts, bias_in, up_bias, size)
    flat = [
        (
            project_in[l].reshape(project_in.shape[1], -1),
            project_out[l].reshape(-1, project_out.shape[3]),
            up_weight[l],
            down_weight[l],
        )
        for l in range(layers)
    ]
    weights = [
        [gather(flat[l][k], COLORS[l % 2][k], FEATURES[k]) for k in range(4)]
        for l in range(layers)
    ]
    values = flipped(inputs.reshape(-1, width), 1, "dp").astype(SINGLE)
    kept = []
    for l in range(layers):
        values, saved = layer_forward(values, small[l], weights[l], size)
        kept.append(saved)
    outputs = flipped(values.astype(NARROW), 1, "dp").reshape(shapes)
    grad = flipped(cotangent.reshape(-1, width), 1, "dp").astype(SINGLE)
    owned = [None] * layers
    parts = [None] * layers
    for l in reversed(range(layers)):
        grad, big, sums = layer_backward(grad, kept[l], small[l], weights[l], size)
        owned[l] = [
            scatter(
                big[k][0], big[k][1], COLORS[l % 2][k], FEATURES[k], flat[l][k].shape[FEATURES[k]]
            )
            for k in range(4)
        ]
        parts[l] = sum_small(sums, (bias_in.shape, up_bias.shape), size)
    input_grad = flipped(grad.astype(NARROW), 1, "dp").reshape(shapes)
    gains, shifts, enter_bias, up_bias_grad = (
        jnp.stack([parts[l][at] for l in range(layers)]) for at in range(4)
    )
    stacked = [jnp.stack([owned[l][k] for l in range(layers)]) for k in range(4)]
    return (
        outputs,
        input_grad,
        gains,
        shifts,
        stacked[0].reshape(project_in.shape),
        enter_bias,
        stacked[1].reshape(project_out.shape),
        stacked[2],
        up_bias_grad,
        stacked[3],
    )


def solution(mesh):
    specs = (
        P(None, ("dp", "tensor"), None),
        P(None, ("dp", "tensor"), None),
        P(None, None, "dp"),
        P(None, None, "dp"),
        P(None, "dp", "tensor", None),
        P(None, "tensor", "dp"),
        P(None, "tensor", None, "dp"),
        P(None, "dp", "tensor"),
        P(None, "tensor", "dp"),
        P(None, "tensor", "dp"),
    )
    return jax.shard_map(step, mesh=mesh, in_specs=specs, out_specs=specs, check_vma=False)
```
